32 devices in a mesh: row: 8 (over y, x, core), col: 4 (over z).
Axes of the slice: x: 2, y: 2, z: 4, core: 2. Of those that a mesh axis runs over, the one named last changes fastest.
Arguments:
- weights: int32 [4096, 4096], P('row', 'col'), may hold values from 1 to 64
Outputs:
- distances: int32 [4096, 4096], P('row', 'col')
The draws below stay inside these ranges and needn't reach their ends.
All inputs are finite; a program needn't handle non-finite values.
Results may differ from the reference program's by a relative error of at most 0.000001.
Values may be sent and summed in bfloat16 or wider, within the bound.
A program may use at most 64 MiB of HBM per device.

```python
import jax
import jax.numpy as jnp
from jax import lax

PIVOT = 128
STEPS = 4
VERTS = 4096
STRIDE = 1024


def set_ends(drawn, rng, low, top_value):
    shape = drawn.shape
    place = [jax.random.randint(jax.random.fold_in(rng, axis), (), 0, shape[axis]) for axis in range(len(shape))]
    drawn = drawn.at[tuple(place)].set(low)
    longest = shape.index(max(shape))
    place[longest] = (place[longest] + 1) % shape[longest]
    return drawn.at[tuple(place)].set(top_value)


def setup_inputs(seed: int = 0) -> dict:
    splits = jax.random.split(jax.random.key(seed), 2)
    weights = set_ends(jax.random.randint(splits[0], (VERTS, VERTS), 1, 65), jax.random.fold_in(splits[0], 1), 1, 64).astype(jnp.int32)
    return {"weights": weights}


def relax(vertex, dist):
    vertex = jnp.asarray(vertex).astype(jnp.int32)
    column = lax.dynamic_slice_in_dim(dist, vertex, 1, 1)
    across = lax.dynamic_slice_in_dim(dist, vertex, 1, 0)
    return jnp.minimum(dist, column + across)


def reference(weights):
    labels = jnp.arange(VERTS, dtype=jnp.int32)
    dist = jnp.where(labels[:, None] == labels[None, :], jnp.int32(0), weights).astype(jnp.int32)
    for step in range(STEPS):
        first = step * STRIDE
        dist = lax.fori_loop(first, first + PIVOT, relax, dist)
    return dist
```

```python
import jax
import jax.numpy as jnp
from jax import lax
from jax.experimental import pallas as pl
from jax.experimental.pallas import tpu as pltpu
from jax.sharding import PartitionSpec as P

PIVOT = 128
STEPS = 4
MESH = pl.DeviceIdType.MESH

BETA = 7.03
SLACK = 0.0021
LOW_LEFT = ((18.09, 0, 36), (0.10, 0, 17))
LOW_RIGHT = ((0.10, 0, 17), (18.09, 18, 36))
LOW_SUM = 18.19
HIGH_LEFT = ((18.09, 0, 36), (35.09, 17, 36), (8.09, 0, 26), (45.09, 37, 63))
HIGH_RIGHT = ((35.09, 17, 53), (18.09, 0, 16), (45.09, 54, 63), (8.09, 0, 26))
HIGH_SUM = 53.18
HIGH_FIRST = 36.0


def window(dist, centre, first, last):
    power = jnp.exp2((centre - dist) * BETA)
    kept = dist <= last if first == 0 else (dist >= first) & (dist <= last)
    return jnp.where(kept, power, 0.0).astype(jnp.bfloat16)


def encode(dist, windows, axis):
    return jnp.concatenate([window(dist, *part) for part in windows], axis=axis)


def encode_left(dist):
    return encode(dist, LOW_LEFT, 1), encode(dist, HIGH_LEFT, 1)


def encode_right(dist):
    return encode(dist, LOW_RIGHT, 0), encode(dist, HIGH_RIGHT, 0)


def product(left, right):
    return jnp.dot(left, right, preferred_element_type=jnp.float32)


def decode(low, high):
    low = (LOW_SUM - SLACK) - jnp.log2(low) * (1.0 / BETA)
    high = (HIGH_SUM - SLACK) - jnp.log2(high) * (1.0 / BETA)
    return jnp.ceil(jnp.minimum(low, jnp.maximum(high, HIGH_FIRST)))


def min_plus(left, right):
    return decode(product(left[0], right[0]), product(left[1], right[1]))


def gather_kernel(n_row, n_col, strip_rows, strip_cols, panel_rows, panel_cols, pivots,
                  send_rows, recv_rows, send_cols, recv_cols, send_piv, recv_piv, local_sem):
    r, c = lax.axis_index("row"), lax.axis_index("col")
    row_gap, col_gap = n_row // STEPS, n_col // STEPS
    barrier = pltpu.get_barrier_semaphore()
    for k in range(1, n_row):
        pl.semaphore_signal(barrier, inc=1, device_id=(lax.rem(r + k, n_row), c), device_id_type=MESH)
    for k in range(1, n_col):
        pl.semaphore_signal(barrier, inc=1, device_id=(r, lax.rem(c + k, n_col)), device_id_type=MESH)
    pl.semaphore_wait(barrier, n_row + n_col - 2)

    def cols_copy(s, k):
        return pltpu.make_async_remote_copy(
            src_ref=strip_cols, dst_ref=panel_cols.at[s],
            send_sem=send_cols.at[k - 1], recv_sem=recv_cols.at[s],
            device_id=(r, lax.rem(c + k, n_col)), device_id_type=MESH)

    def rows_copy(s, k):
        return pltpu.make_async_remote_copy(
            src_ref=strip_rows, dst_ref=panel_rows.at[s],
            send_sem=send_rows.at[k - 1], recv_sem=recv_rows.at[s],
            device_id=(lax.rem(r + k, n_row), c), device_id_type=MESH)

    def piv_copy(s, k):
        return pltpu.make_async_remote_copy(
            src_ref=panel_cols.at[:, pl.ds(0, PIVOT)], dst_ref=pivots.at[s],
            send_sem=send_piv.at[k - 1], recv_sem=recv_piv.at[s],
            device_id=(lax.rem(r + k, n_row), c), device_id_type=MESH)

    for s in range(STEPS):
        @pl.when(c == s * col_gap)
        def _():
            for k in range(1, n_col):
                cols_copy(s, k).start()
            own = pltpu.make_async_copy(strip_cols, panel_cols.at[s], local_sem.at[0])
            own.start()
            own.wait()

    for s in range(STEPS):
        @pl.when(r == s * row_gap)
        def _():
            for k in range(1, n_row):
                rows_copy(s, k).start()
            own = pltpu.make_async_copy(strip_rows, panel_rows.at[s], local_sem.at[1])
            own.start()
            own.wait()

    for s in range(STEPS):
        @pl.when(c != s * col_gap)
        def _():
            cols_copy(s, 1).wait_recv()

    for s in range(STEPS):
        @pl.when(r == s * row_gap)
        def _():
            for k in range(1, n_row):
                piv_copy(s, k).start()
            own = pltpu.make_async_copy(panel_cols.at[:, pl.ds(0, PIVOT)], pivots.at[s], local_sem.at[2])
            own.start()
            own.wait()

    for s in range(STEPS):
        @pl.when(r != s * row_gap)
        def _():
            rows_copy(s, 1).wait_recv()
            piv_copy(s, 1).wait_recv()

    for s in range(STEPS):
        @pl.when(c == s * col_gap)
        def _():
            for k in range(1, n_col):
                cols_copy(s, k).wait_send()

        @pl.when(r == s * row_gap)
        def _():
            for k in range(1, n_row):
                rows_copy(s, k).wait_send()
                piv_copy(s, k).wait_send()


def gather(n_row, n_col, strip_rows, strip_cols):
    rows_dev, cols_dev = strip_cols.shape[0], strip_rows.shape[1]
    vmem = pl.BlockSpec(memory_space=pltpu.VMEM)
    dma = pltpu.SemaphoreType.DMA
    return pl.pallas_call(
        lambda *refs: gather_kernel(n_row, n_col, *refs),
        out_shape=(
            jax.ShapeDtypeStruct((STEPS, PIVOT, cols_dev), jnp.bfloat16),
            jax.ShapeDtypeStruct((STEPS, rows_dev, PIVOT), jnp.bfloat16),
            jax.ShapeDtypeStruct((STEPS, STEPS, PIVOT, PIVOT), jnp.bfloat16),
        ),
        in_specs=[vmem] * 2,
        out_specs=(vmem,) * 3,
        scratch_shapes=[
            dma((n_row - 1,)), dma((STEPS,)), dma((n_col - 1,)), dma((STEPS,)),
            dma((n_row - 1,)), dma((STEPS,)), dma((3,)),
        ],
        compiler_params=pltpu.CompilerParams(collective_id=0, has_side_effects=True),
    )(strip_rows, strip_cols)


def close_block(block):
    def more(state):
        return (state[0] < 6) & state[1]

    def square(state):
        count, _, now = state
        new = jnp.minimum(now, min_plus(encode_left(now), encode_right(now)))
        return count + 1, jnp.max(now - new) > 0.5, new

    return lax.while_loop(more, square, (jnp.int32(0), jnp.bool_(True), block))[2]


def close_kernel(panel_cols, pivots, closed, dist):
    size = STEPS * PIVOT
    rows = panel_cols.shape[1]
    tile = 256
    for s in range(STEPS):
        for t in range(STEPS):
            dist[s * PIVOT : (s + 1) * PIVOT, t * PIVOT : (t + 1) * PIVOT] = pivots[s, t].astype(jnp.float32)
        dist[size : size + rows, s * PIVOT : (s + 1) * PIVOT] = panel_cols[s].astype(jnp.float32)
    for s in range(STEPS):
        mine = slice(s * PIVOT, (s + 1) * PIVOT)
        block = close_block(dist[mine, mine])
        block_right = encode_right(block)
        across_right = encode_right(dist[mine, :])

        def update(index, carry):
            part = pl.ds(pl.multiple_of(index * tile, tile), tile)
            column = min_plus(encode_left(dist[part, mine]), block_right)
            dist[part, :] = jnp.minimum(dist[part, :], min_plus(encode_left(column), across_right))
            return carry

        lax.fori_loop(0, (size + rows) // tile, update, 0)
    for s in range(STEPS):
        closed[s] = dist[size : size + rows, s * PIVOT : (s + 1) * PIVOT].astype(jnp.bfloat16)


def close(panel_cols, pivots):
    rows = panel_cols.shape[1]
    vmem = pl.BlockSpec(memory_space=pltpu.VMEM)
    return pl.pallas_call(
        close_kernel,
        out_shape=jax.ShapeDtypeStruct(panel_cols.shape, jnp.bfloat16),
        in_specs=[vmem] * 2,
        out_specs=vmem,
        scratch_shapes=[pltpu.VMEM((STEPS * PIVOT + rows, STEPS * PIVOT), jnp.float32)],
    )(panel_cols, pivots)


def finish_kernel(offset, closed, panel_rows, weights, out, low_right, high_right, low_left, high_left):
    tile, cols = weights.shape
    wide = 256

    @pl.when(pl.program_id(0) == 0)
    def _():
        def one(index, carry):
            s, part = index // (cols // wide), index % (cols // wide)
            where = pl.ds(pl.multiple_of(part * wide, wide), wide)
            low, high = encode_right(panel_rows[s, :, where].astype(jnp.float32))
            low_right[s, :, where] = low
            high_right[s, :, where] = high
            return carry

        lax.fori_loop(0, STEPS * (cols // wide), one, 0)

    for s in range(STEPS):
        low, high = encode_left(closed[s].astype(jnp.float32))
        low_left[s] = low
        high_left[s] = high

    base = offset[0] + pl.program_id(0) * tile

    def columns(index, carry):
        start = pl.multiple_of(index * wide, wide)
        where = pl.ds(start, wide)
        low = product(low_left[0], low_right[0, :, where])
        high = product(high_left[0], high_right[0, :, where])
        for s in range(1, STEPS):
            low = jnp.maximum(low, product(low_left[s], low_right[s, :, where]))
            high = jnp.maximum(high, product(high_left[s], high_right[s, :, where]))
        shape = (tile, wide)
        gap = lax.broadcasted_iota(jnp.int32, shape, 0) - lax.broadcasted_iota(jnp.int32, shape, 1)
        old = jnp.where(gap == start - base, 0, weights[:, where])
        best = jnp.minimum(decode(low, high), 64.0).astype(jnp.int32)
        out[:, where] = jnp.minimum(old, best)
        return carry

    lax.fori_loop(0, cols // wide, columns, 0)


def finish(offset, closed, panel_rows, weights):
    rows, cols = weights.shape
    tile = 256
    return pl.pallas_call(
        finish_kernel,
        out_shape=jax.ShapeDtypeStruct(weights.shape, jnp.int32),
        grid=(rows // tile,),
        in_specs=[
            pl.BlockSpec(memory_space=pltpu.SMEM),
            pl.BlockSpec((STEPS, tile, PIVOT), lambda i: (0, i, 0)),
            pl.BlockSpec((STEPS, PIVOT, cols), lambda i: (0, 0, 0)),
            pl.BlockSpec((tile, cols), lambda i: (i, 0)),
        ],
        out_specs=pl.BlockSpec((tile, cols), lambda i: (i, 0)),
        scratch_shapes=[
            pltpu.VMEM((STEPS, 2 * PIVOT, cols), jnp.bfloat16),
            pltpu.VMEM((STEPS, 4 * PIVOT, cols), jnp.bfloat16),
            pltpu.VMEM((STEPS, tile, 2 * PIVOT), jnp.bfloat16),
            pltpu.VMEM((STEPS, tile, 4 * PIVOT), jnp.bfloat16),
        ],
    )(offset, closed, panel_rows, weights)


def solution(mesh):
    n_row, n_col = mesh.shape["row"], mesh.shape["col"]
    assert n_row % STEPS == 0 and n_col % STEPS == 0

    def per_device(weights):
        rows_dev, cols_dev = weights.shape
        offset = lax.axis_index("row") * rows_dev - lax.axis_index("col") * cols_dev
        down = jnp.arange(rows_dev, dtype=jnp.int32)[:, None] + offset
        across = jnp.arange(cols_dev, dtype=jnp.int32)[None, :]

        def strip(height, width):
            kept = weights[:height, :width]
            return jnp.where(down[:height] == across[:, :width], 0, kept).astype(jnp.bfloat16)

        panel_rows, panel_cols, pivots = gather(
            n_row, n_col, strip(PIVOT, cols_dev), strip(rows_dev, PIVOT))
        closed = close(panel_cols, pivots)
        return finish(jnp.full((1,), offset, jnp.int32), closed, panel_rows, weights)

    return jax.shard_map(
        per_device, mesh=mesh, in_specs=(P("row", "col"),), out_specs=P("row", "col"), check_vma=False)
```

```python
import jax
import jax.numpy as jnp
from jax import lax
from jax.experimental import pallas as pl
from jax.experimental.pallas import tpu as pltpu
from jax.sharding import PartitionSpec as P

PIVOT = 128
STEPS = 4
MESH = pl.DeviceIdType.MESH

BETA = 7.03
SLACK = 0.0021
LOW_SUM = 18.19
HIGH_LEFT = ((18.09, 0, 36), (35.09, 17, 36), (8.09, 0, 26), (45.09, 37, 63))
HIGH_RIGHT = ((35.09, 17, 53), (18.09, 0, 16), (45.09, 54, 63), (8.09, 0, 26))
HIGH_SUM = 53.18
HIGH_FIRST = 36.0


def step_of(centre, base):
    return 2.0 ** (BETA * (centre - base))


def power(scaled, centre):
    return jnp.exp2(BETA * centre - scaled)


def keep(value, dist, first, last):
    kept = dist <= last if first == 0 else (dist >= first) & (dist <= last)
    return jnp.where(kept, value, 0.0).astype(jnp.bfloat16)


def encode_left(dist):
    scaled = dist * BETA
    p18 = power(scaled, 18.09)
    p08 = p18 * step_of(8.09, 18.09)
    first = keep(p18, dist, 0, 36)
    low = [first, keep(p08 * step_of(0.10, 8.09), dist, 0, 17)]
    high = [first, keep(p18 * step_of(35.09, 18.09), dist, 17, 36), keep(p08, dist, 0, 26),
            keep(power(scaled, 45.09), dist, 37, 63)]
    return jnp.concatenate(low, axis=1), jnp.concatenate(high, axis=1)


def encode_right(dist):
    scaled = dist * BETA
    p18 = power(scaled, 18.09)
    p08 = p18 * step_of(8.09, 18.09)
    low = [keep(p08 * step_of(0.10, 8.09), dist, 0, 17), keep(p18, dist, 18, 36)]
    high = [keep(power(scaled, 35.09), dist, 17, 53), keep(p18, dist, 0, 16),
            keep(power(scaled, 45.09), dist, 54, 63), keep(p08, dist, 0, 26)]
    return jnp.concatenate(low, axis=0), jnp.concatenate(high, axis=0)


def product(left, right):
    return jnp.dot(left, right, preferred_element_type=jnp.float32)


def decode(low, high):
    low = (LOW_SUM - SLACK) - jnp.log2(low) * (1.0 / BETA)
    high = (HIGH_SUM - SLACK) - jnp.log2(high) * (1.0 / BETA)
    return jnp.ceil(jnp.minimum(low, jnp.maximum(high, HIGH_FIRST)))


def min_plus(left, right):
    return decode(product(left[0], right[0]), product(left[1], right[1]))


def strips_kernel(offset, rows, cols, strip_rows, strip_cols):
    for part, strip in ((rows, strip_rows), (cols, strip_cols)):
        gap = lax.broadcasted_iota(jnp.int32, part.shape, 0) - lax.broadcasted_iota(jnp.int32, part.shape, 1)
        kept = jnp.where(gap == -offset[0], 0, part[...])
        strip[...] = kept.astype(jnp.float32).astype(jnp.bfloat16)


def strips(offset, weights):
    rows, cols = weights.shape
    corner = lambda shape: pl.BlockSpec(shape, lambda i: (0, 0))
    shapes = (PIVOT, cols), (rows, PIVOT)
    return pl.pallas_call(
        strips_kernel,
        out_shape=tuple(jax.ShapeDtypeStruct(shape, jnp.bfloat16) for shape in shapes),
        grid=(1,),
        in_specs=[pl.BlockSpec(memory_space=pltpu.SMEM)] + [corner(shape) for shape in shapes],
        out_specs=tuple(corner(shape) for shape in shapes),
    )(offset, weights, weights)


def close_block(block):
    def square(_, now):
        return jnp.minimum(now, min_plus(encode_left(now), encode_right(now)))

    return lax.fori_loop(0, 6, square, block)


def gather_close_kernel(n_row, n_col, strip_rows, strip_cols, panel_rows, closed,
                        panel_cols, pivots, dist, low_right, high_right,
                        send_piv, recv_piv, pass_piv, send_rows, recv_rows, pass_rows,
                        send_cols, recv_cols, local_sem):
    r, c = lax.axis_index("row"), lax.axis_index("col")
    row_gap, col_gap = n_row // STEPS, n_col // STEPS
    leader = lax.rem(r, row_gap) == 0
    group = r // row_gap
    rows_dev = strip_cols.shape[0]
    barrier = pltpu.get_barrier_semaphore()
    for k in range(1, n_row):
        pl.semaphore_signal(barrier, inc=1, device_id=(lax.rem(r + k, n_row), c), device_id_type=MESH)
    for k in range(1, n_col):
        pl.semaphore_signal(barrier, inc=1, device_id=(r, lax.rem(c + k, n_col)), device_id_type=MESH)
    pl.semaphore_wait(barrier, n_row + n_col - 2)

    parts = pl.ds(0, PIVOT), pl.ds(PIVOT, rows_dev - PIVOT)

    def cols_copy(s, part, k):
        return pltpu.make_async_remote_copy(
            src_ref=strip_cols.at[parts[part]], dst_ref=panel_cols.at[s, parts[part]],
            send_sem=send_cols.at[part, k - 1], recv_sem=recv_cols.at[part, s],
            device_id=(r, lax.rem(c + k, n_col)), device_id_type=MESH)

    def cols_own(s, part):
        return pltpu.make_async_copy(
            strip_cols.at[parts[part]], panel_cols.at[s, parts[part]], local_sem.at[part])

    def to_leader(src, dst, s, k, send, recv):
        return pltpu.make_async_remote_copy(
            src_ref=src, dst_ref=dst.at[s], send_sem=send.at[k - 1], recv_sem=recv.at[s],
            device_id=(lax.rem(r + k * row_gap, n_row), c), device_id_type=MESH)

    def to_member(src, dst, s, m, send, recv):
        return pltpu.make_async_remote_copy(
            src_ref=src, dst_ref=dst.at[s], send_sem=send.at[s, m - 1], recv_sem=recv.at[s],
            device_id=(r + m, c), device_id_type=MESH)

    corner = panel_cols.at[:, parts[0]]
    piv = pivots, send_piv, recv_piv
    row = panel_rows, send_rows, recv_rows

    for s in range(STEPS):
        @pl.when(c == s * col_gap)
        def _():
            @pl.when(leader)
            def _():
                for k in range(1, n_col):
                    cols_copy(s, 0, k).start()
            cols_own(s, 0).start()
            cols_own(s, 1).start()
            cols_own(s, 0).wait()
            cols_own(s, 1).wait()

    for s in range(STEPS):
        @pl.when(leader & (c != s * col_gap))
        def _():
            cols_copy(s, 0, 1).wait_recv()

    for s in range(STEPS):
        @pl.when(leader & (group == s))
        def _():
            for k in range(1, STEPS):
                to_leader(corner, pivots, s, k, send_piv, recv_piv).start()
            for m in range(1, row_gap):
                to_member(corner, pivots, s, m, pass_piv, recv_piv).start()
            for k in range(1, STEPS):
                to_leader(strip_rows, panel_rows, s, k, send_rows, recv_rows).start()
            for m in range(1, row_gap):
                to_member(strip_rows, panel_rows, s, m, pass_rows, recv_rows).start()
            own_piv = pltpu.make_async_copy(corner, pivots.at[s], local_sem.at[0])
            own_row = pltpu.make_async_copy(strip_rows, panel_rows.at[s], local_sem.at[1])
            own_piv.start()
            own_row.start()
            own_piv.wait()
            own_row.wait()

    for s in range(STEPS):
        @pl.when(leader & (c == s * col_gap))
        def _():
            for k in range(1, n_col):
                cols_copy(s, 1, k).start()

    def pass_on(dst, passing, send, recv):
        for j in range(1, STEPS):
            s = lax.rem(group + j, STEPS)

            @pl.when(leader)
            def _():
                to_leader(dst.at[0], dst, s, 1, send, recv).wait_recv()
                for m in range(1, row_gap):
                    to_member(dst.at[s], dst, s, m, passing, recv).start()

    pass_on(pivots, pass_piv, send_piv, recv_piv)

    @pl.when(jnp.logical_not(leader))
    def _():
        for s in range(STEPS):
            to_member(pivots.at[s], pivots, s, 1, pass_piv, recv_piv).wait_recv()

    for s in range(STEPS):
        @pl.when(jnp.logical_not(leader) & (c == s * col_gap))
        def _():
            for part in range(2):
                for k in range(1, n_col):
                    cols_copy(s, part, k).start()

    size = STEPS * PIVOT
    for s in range(STEPS):
        for t in range(STEPS):
            dist[s * PIVOT : (s + 1) * PIVOT, t * PIVOT : (t + 1) * PIVOT] = pivots[s, t].astype(jnp.float32)
    for s in range(STEPS):
        mine = slice(s * PIVOT, (s + 1) * PIVOT)
        block = close_block(dist[mine, mine])
        column = min_plus(encode_left(dist[:, mine]), encode_right(block))
        dist[...] = jnp.minimum(dist[...], min_plus(encode_left(column), encode_right(dist[mine, :])))
        if s == STEPS // 2 - 1:
            pass_on(panel_rows, pass_rows, send_rows, recv_rows)

    for s in range(STEPS):
        low, high = encode_right(dist[s * PIVOT : (s + 1) * PIVOT, :])
        low_right[s] = low
        high_right[s] = high

    for s in range(STEPS):
        @pl.when(c != s * col_gap)
        def _():
            cols_copy(s, 1, 1).wait_recv()

        @pl.when(jnp.logical_not(leader) & (c != s * col_gap))
        def _():
            cols_copy(s, 0, 1).wait_recv()

    tile = 256

    def update(index, carry):
        part = pl.ds(pl.multiple_of(index * tile, tile), tile)
        low = high = None
        for s in range(STEPS):
            left = encode_left(panel_cols[s, part, :].astype(jnp.float32))
            one, two = product(left[0], low_right[s]), product(left[1], high_right[s])
            low = one if s == 0 else jnp.maximum(low, one)
            high = two if s == 0 else jnp.maximum(high, two)
        best = jnp.minimum(decode(low, high), 64.0).astype(jnp.bfloat16)
        for s in range(STEPS):
            closed[s, part, :] = best[:, s * PIVOT : (s + 1) * PIVOT]
        return carry

    lax.fori_loop(0, rows_dev // tile, update, 0)

    @pl.when(jnp.logical_not(leader))
    def _():
        for s in range(STEPS):
            to_member(panel_rows.at[s], panel_rows, s, 1, pass_rows, recv_rows).wait_recv()

    for s in range(STEPS):
        @pl.when(c == s * col_gap)
        def _():
            for part in range(2):
                for k in range(1, n_col):
                    cols_copy(s, part, k).wait_send()

        @pl.when(leader)
        def _():
            for m in range(1, row_gap):
                to_member(pivots.at[s], pivots, s, m, pass_piv, recv_piv).wait_send()
                to_member(panel_rows.at[s], panel_rows, s, m, pass_rows, recv_rows).wait_send()

    @pl.when(leader)
    def _():
        for k in range(1, STEPS):
            to_leader(corner, pivots, 0, k, send_piv, recv_piv).wait_send()
            to_leader(strip_rows, panel_rows, 0, k, send_rows, recv_rows).wait_send()


def gather_close(n_row, n_col, strip_rows, strip_cols):
    rows_dev, cols_dev = strip_cols.shape[0], strip_rows.shape[1]
    vmem = pl.BlockSpec(memory_space=pltpu.VMEM)
    dma = pltpu.SemaphoreType.DMA
    size = STEPS * PIVOT
    members = max(n_row // STEPS - 1, 1)
    return pl.pallas_call(
        lambda *refs: gather_close_kernel(n_row, n_col, *refs),
        out_shape=(
            jax.ShapeDtypeStruct((STEPS, PIVOT, cols_dev), jnp.bfloat16),
            jax.ShapeDtypeStruct((STEPS, rows_dev, PIVOT), jnp.bfloat16),
        ),
        in_specs=[vmem] * 2,
        out_specs=(vmem,) * 2,
        scratch_shapes=[
            pltpu.VMEM((STEPS, rows_dev, PIVOT), jnp.bfloat16),
            pltpu.VMEM((STEPS, STEPS, PIVOT, PIVOT), jnp.bfloat16),
            pltpu.VMEM((size, size), jnp.float32),
            pltpu.VMEM((STEPS, 2 * PIVOT, size), jnp.bfloat16),
            pltpu.VMEM((STEPS, 4 * PIVOT, size), jnp.bfloat16),
            dma((STEPS - 1,)), dma((STEPS,)), dma((STEPS, members)),
            dma((STEPS - 1,)), dma((STEPS,)), dma((STEPS, members)),
            dma((2, n_col - 1)), dma((2, STEPS)), dma((2,)),
        ],
        compiler_params=pltpu.CompilerParams(collective_id=0, has_side_effects=True),
    )(strip_rows, strip_cols)


def finish_kernel(offset, closed, panel_rows, weights, out, low_right, high_right, low_left, high_left):
    tile, cols = weights.shape
    wide = 256

    @pl.when(pl.program_id(0) == 0)
    def _():
        def one(index, carry):
            s, part = index // (cols // wide), index % (cols // wide)
            where = pl.ds(pl.multiple_of(part * wide, wide), wide)
            low, high = encode_right(panel_rows[s, :, where].astype(jnp.float32))
            low_right[s, :, where] = low
            high_right[s, :, where] = high
            return carry

        lax.fori_loop(0, STEPS * (cols // wide), one, 0)

    for s in range(STEPS):
        low, high = encode_left(closed[s].astype(jnp.float32))
        low_left[s] = low
        high_left[s] = high

    base = offset[0] + pl.program_id(0) * tile

    def columns(index, carry):
        start = pl.multiple_of(index * wide, wide)
        where = pl.ds(start, wide)
        low = product(low_left[0], low_right[0, :, where])
        high = product(high_left[0], high_right[0, :, where])
        for s in range(1, STEPS):
            low = jnp.maximum(low, product(low_left[s], low_right[s, :, where]))
            high = jnp.maximum(high, product(high_left[s], high_right[s, :, where]))
        shape = (tile, wide)
        gap = lax.broadcasted_iota(jnp.int32, shape, 0) - lax.broadcasted_iota(jnp.int32, shape, 1)
        old = jnp.where(gap == start - base, 0, weights[:, where])
        best = jnp.minimum(decode(low, high), 64.0).astype(jnp.int32)
        out[:, where] = jnp.minimum(old, best)
        return carry

    lax.fori_loop(0, cols // wide, columns, 0)


def finish(offset, closed, panel_rows, weights):
    rows, cols = weights.shape
    tile = 256
    return pl.pallas_call(
        finish_kernel,
        out_shape=jax.ShapeDtypeStruct(weights.shape, jnp.int32),
        grid=(rows // tile,),
        in_specs=[
            pl.BlockSpec(memory_space=pltpu.SMEM),
            pl.BlockSpec((STEPS, tile, PIVOT), lambda i: (0, i, 0)),
            pl.BlockSpec((STEPS, PIVOT, cols), lambda i: (0, 0, 0)),
            pl.BlockSpec((tile, cols), lambda i: (i, 0)),
        ],
        out_specs=pl.BlockSpec((tile, cols), lambda i: (i, 0)),
        scratch_shapes=[
            pltpu.VMEM((STEPS, 2 * PIVOT, cols), jnp.bfloat16),
            pltpu.VMEM((STEPS, 4 * PIVOT, cols), jnp.bfloat16),
            pltpu.VMEM((STEPS, tile, 2 * PIVOT), jnp.bfloat16),
            pltpu.VMEM((STEPS, tile, 4 * PIVOT), jnp.bfloat16),
        ],
    )(offset, closed, panel_rows, weights)


def solution(mesh):
    n_row, n_col = mesh.shape["row"], mesh.shape["col"]
    assert n_row % STEPS == 0 and n_col % STEPS == 0

    def per_device(weights):
        rows_dev, cols_dev = weights.shape
        offset = lax.axis_index("row") * rows_dev - lax.axis_index("col") * cols_dev
        offset = jnp.full((1,), offset, jnp.int32)
        panel_rows, closed = gather_close(n_row, n_col, *strips(offset, weights))
        return finish(offset, closed, panel_rows, weights)

    return jax.shard_map(
        per_device, mesh=mesh, in_specs=(P("row", "col"),), out_specs=P("row", "col"), check_vma=False)
```

```python
import jax
import jax.numpy as jnp
from jax import lax
from jax.experimental import pallas as pl
from jax.experimental.pallas import tpu as pltpu
from jax.sharding import PartitionSpec as P

PIVOT = 128
STEPS = 4
MESH = pl.DeviceIdType.MESH

BETA = 7.03
SLACK = 0.0021
LOW_SUM = 18.19
HIGH_LEFT = ((18.09, 0, 36), (35.09, 17, 36), (8.09, 0, 26), (45.09, 37, 63))
HIGH_RIGHT = ((35.09, 17, 53), (18.09, 0, 16), (45.09, 54, 63), (8.09, 0, 26))
HIGH_SUM = 53.18
HIGH_FIRST = 36.0


def step_of(centre, base):
    return 2.0 ** (BETA * (centre - base))


def power(scaled, centre):
    return jnp.exp2(BETA * centre - scaled)


def keep(value, dist, first, last):
    dist = dist.astype(jnp.bfloat16)
    kept = dist <= last if first == 0 else (dist >= first) & (dist <= last)
    return jnp.where(kept, value.astype(jnp.bfloat16), jnp.bfloat16(0))


def encode_left(dist):
    scaled = dist * BETA
    p18 = power(scaled, 18.09)
    p08 = p18 * step_of(8.09, 18.09)
    first = keep(p18, dist, 0, 36)
    low = [first, keep(p08 * step_of(0.10, 8.09), dist, 0, 17)]
    high = [first, keep(p18 * step_of(35.09, 18.09), dist, 17, 36), keep(p08, dist, 0, 26),
            keep(power(scaled, 45.09), dist, 37, 63)]
    return jnp.concatenate(low, axis=1), jnp.concatenate(high, axis=1)


def encode_right(dist):
    scaled = dist * BETA
    p18 = power(scaled, 18.09)
    p08 = p18 * step_of(8.09, 18.09)
    low = [keep(p08 * step_of(0.10, 8.09), dist, 0, 17), keep(p18, dist, 18, 36)]
    high = [keep(power(scaled, 35.09), dist, 17, 53), keep(p18, dist, 0, 16),
            keep(power(scaled, 45.09), dist, 54, 63), keep(p08, dist, 0, 26)]
    return jnp.concatenate(low, axis=0), jnp.concatenate(high, axis=0)


def product(left, right):
    return jnp.dot(left, right, preferred_element_type=jnp.float32)


def decode(low, high):
    low = (LOW_SUM - SLACK) - jnp.log2(low) * (1.0 / BETA)
    high = (HIGH_SUM - SLACK) - jnp.log2(high) * (1.0 / BETA)
    return jnp.ceil(jnp.minimum(low, jnp.maximum(high, HIGH_FIRST)))


def min_plus(left, right):
    return decode(product(left[0], right[0]), product(left[1], right[1]))


def strips_kernel(offset, rows, cols, strip_rows, strip_cols):
    for part, strip in ((rows, strip_rows), (cols, strip_cols)):
        gap = lax.broadcasted_iota(jnp.int32, part.shape, 0) - lax.broadcasted_iota(jnp.int32, part.shape, 1)
        kept = jnp.where(gap == -offset[0], 0, part[...])
        strip[...] = kept.astype(jnp.float32).astype(jnp.bfloat16)


def strips(offset, weights):
    rows, cols = weights.shape
    corner = lambda shape: pl.BlockSpec(shape, lambda i: (0, 0))
    shapes = (PIVOT, cols), (rows, PIVOT)
    return pl.pallas_call(
        strips_kernel,
        out_shape=tuple(jax.ShapeDtypeStruct(shape, jnp.bfloat16) for shape in shapes),
        grid=(1,),
        in_specs=[pl.BlockSpec(memory_space=pltpu.SMEM)] + [corner(shape) for shape in shapes],
        out_specs=tuple(corner(shape) for shape in shapes),
    )(offset, weights, weights)


def close_block(block):
    def square(_, now):
        return jnp.minimum(now, min_plus(encode_left(now), encode_right(now)))

    return lax.fori_loop(0, 6, square, block)


def gather_close_kernel(n_row, n_col, strip_rows, strip_cols, panel_rows, closed,
                        panel_cols, pivots, dist, low_right, high_right,
                        send_piv, recv_piv, pass_piv, send_rows, recv_rows, pass_rows,
                        send_cols, recv_cols, local_sem):
    r, c = lax.axis_index("row"), lax.axis_index("col")
    row_gap, col_gap = n_row // STEPS, n_col // STEPS
    leader = lax.rem(r, row_gap) == 0
    group = r // row_gap
    rows_dev = strip_cols.shape[0]
    barrier = pltpu.get_barrier_semaphore()
    for k in range(1, n_row):
        pl.semaphore_signal(barrier, inc=1, device_id=(lax.rem(r + k, n_row), c), device_id_type=MESH)
    for k in range(1, n_col):
        pl.semaphore_signal(barrier, inc=1, device_id=(r, lax.rem(c + k, n_col)), device_id_type=MESH)
    pl.semaphore_wait(barrier, n_row + n_col - 2)

    parts = pl.ds(0, PIVOT), pl.ds(PIVOT, rows_dev - PIVOT)

    def cols_copy(s, part, k):
        return pltpu.make_async_remote_copy(
            src_ref=strip_cols.at[parts[part]], dst_ref=panel_cols.at[s, parts[part]],
            send_sem=send_cols.at[part, k - 1], recv_sem=recv_cols.at[part, s],
            device_id=(r, lax.rem(c + k, n_col)), device_id_type=MESH)

    def cols_own(s, part):
        return pltpu.make_async_copy(
            strip_cols.at[parts[part]], panel_cols.at[s, parts[part]], local_sem.at[part])

    def to_leader(src, dst, s, k, send, recv):
        return pltpu.make_async_remote_copy(
            src_ref=src, dst_ref=dst.at[s], send_sem=send.at[k - 1], recv_sem=recv.at[s],
            device_id=(lax.rem(r + k * row_gap, n_row), c), device_id_type=MESH)

    def to_member(src, dst, s, m, send, recv):
        return pltpu.make_async_remote_copy(
            src_ref=src, dst_ref=dst.at[s], send_sem=send.at[s, m - 1], recv_sem=recv.at[s],
            device_id=(r + m, c), device_id_type=MESH)

    corner = panel_cols.at[:, parts[0]]
    piv = pivots, send_piv, recv_piv
    row = panel_rows, send_rows, recv_rows

    for s in range(STEPS):
        @pl.when(c == s * col_gap)
        def _():
            @pl.when(leader)
            def _():
                for k in range(1, n_col):
                    cols_copy(s, 0, k).start()
            cols_own(s, 0).start()
            cols_own(s, 1).start()
            cols_own(s, 0).wait()
            cols_own(s, 1).wait()

    for s in range(STEPS):
        @pl.when(leader & (c != s * col_gap))
        def _():
            cols_copy(s, 0, 1).wait_recv()

    for s in range(STEPS):
        @pl.when(leader & (group == s))
        def _():
            for k in range(1, STEPS):
                to_leader(corner, pivots, s, k, send_piv, recv_piv).start()
            for m in range(1, row_gap):
                to_member(corner, pivots, s, m, pass_piv, recv_piv).start()
            for k in range(1, STEPS):
                to_leader(strip_rows, panel_rows, s, k, send_rows, recv_rows).start()
            for m in range(1, row_gap):
                to_member(strip_rows, panel_rows, s, m, pass_rows, recv_rows).start()
            own_piv = pltpu.make_async_copy(corner, pivots.at[s], local_sem.at[0])
            own_row = pltpu.make_async_copy(strip_rows, panel_rows.at[s], local_sem.at[1])
            own_piv.start()
            own_row.start()
            own_piv.wait()
            own_row.wait()

    for s in range(STEPS):
        @pl.when(leader & (c == s * col_gap))
        def _():
            for k in range(1, n_col):
                cols_copy(s, 1, k).start()

    def pass_on(dst, passing, send, recv):
        for j in range(1, STEPS):
            s = lax.rem(group + j, STEPS)

            @pl.when(leader)
            def _():
                to_leader(dst.at[0], dst, s, 1, send, recv).wait_recv()
                for m in range(1, row_gap):
                    to_member(dst.at[s], dst, s, m, passing, recv).start()

    pass_on(pivots, pass_piv, send_piv, recv_piv)

    @pl.when(jnp.logical_not(leader))
    def _():
        for s in range(STEPS):
            to_member(pivots.at[s], pivots, s, 1, pass_piv, recv_piv).wait_recv()

    for s in range(STEPS):
        @pl.when(jnp.logical_not(leader) & (c == s * col_gap))
        def _():
            for part in range(2):
                for k in range(1, n_col):
                    cols_copy(s, part, k).start()

    size = STEPS * PIVOT
    for s in range(STEPS):
        for t in range(STEPS):
            dist[s * PIVOT : (s + 1) * PIVOT, t * PIVOT : (t + 1) * PIVOT] = pivots[s, t].astype(jnp.float32)
    for s in range(STEPS):
        mine = slice(s * PIVOT, (s + 1) * PIVOT)
        block = close_block(dist[mine, mine])
        column = min_plus(encode_left(dist[:, mine]), encode_right(block))
        dist[...] = jnp.minimum(dist[...], min_plus(encode_left(column), encode_right(dist[mine, :])))
        if s == STEPS // 2 - 1:
            pass_on(panel_rows, pass_rows, send_rows, recv_rows)

    for s in range(STEPS):
        low, high = encode_right(dist[s * PIVOT : (s + 1) * PIVOT, :])
        low_right[s] = low
        high_right[s] = high

    for s in range(STEPS):
        @pl.when(c != s * col_gap)
        def _():
            cols_copy(s, 1, 1).wait_recv()

        @pl.when(jnp.logical_not(leader) & (c != s * col_gap))
        def _():
            cols_copy(s, 0, 1).wait_recv()

    tile = 256

    def update(index, carry):
        part = pl.ds(pl.multiple_of(index * tile, tile), tile)
        low = high = None
        for s in range(STEPS):
            left = encode_left(panel_cols[s, part, :].astype(jnp.float32))
            one, two = product(left[0], low_right[s]), product(left[1], high_right[s])
            low = one if s == 0 else jnp.maximum(low, one)
            high = two if s == 0 else jnp.maximum(high, two)
        best = jnp.minimum(decode(low, high), 64.0).astype(jnp.bfloat16)
        for s in range(STEPS):
            closed[s, part, :] = best[:, s * PIVOT : (s + 1) * PIVOT]
        return carry

    lax.fori_loop(0, rows_dev // tile, update, 0)

    @pl.when(jnp.logical_not(leader))
    def _():
        for s in range(STEPS):
            to_member(panel_rows.at[s], panel_rows, s, 1, pass_rows, recv_rows).wait_recv()

    for s in range(STEPS):
        @pl.when(c == s * col_gap)
        def _():
            for part in range(2):
                for k in range(1, n_col):
                    cols_copy(s, part, k).wait_send()

        @pl.when(leader)
        def _():
            for m in range(1, row_gap):
                to_member(pivots.at[s], pivots, s, m, pass_piv, recv_piv).wait_send()
                to_member(panel_rows.at[s], panel_rows, s, m, pass_rows, recv_rows).wait_send()

    @pl.when(leader)
    def _():
        for k in range(1, STEPS):
            to_leader(corner, pivots, 0, k, send_piv, recv_piv).wait_send()
            to_leader(strip_rows, panel_rows, 0, k, send_rows, recv_rows).wait_send()


def gather_close(n_row, n_col, strip_rows, strip_cols):
    rows_dev, cols_dev = strip_cols.shape[0], strip_rows.shape[1]
    vmem = pl.BlockSpec(memory_space=pltpu.VMEM)
    dma = pltpu.SemaphoreType.DMA
    size = STEPS * PIVOT
    members = max(n_row // STEPS - 1, 1)
    return pl.pallas_call(
        lambda *refs: gather_close_kernel(n_row, n_col, *refs),
        out_shape=(
            jax.ShapeDtypeStruct((STEPS, PIVOT, cols_dev), jnp.bfloat16),
            jax.ShapeDtypeStruct((STEPS, rows_dev, PIVOT), jnp.bfloat16),
        ),
        in_specs=[vmem] * 2,
        out_specs=(vmem,) * 2,
        scratch_shapes=[
            pltpu.VMEM((STEPS, rows_dev, PIVOT), jnp.bfloat16),
            pltpu.VMEM((STEPS, STEPS, PIVOT, PIVOT), jnp.bfloat16),
            pltpu.VMEM((size, size), jnp.float32),
            pltpu.VMEM((STEPS, 2 * PIVOT, size), jnp.bfloat16),
            pltpu.VMEM((STEPS, 4 * PIVOT, size), jnp.bfloat16),
            dma((STEPS - 1,)), dma((STEPS,)), dma((STEPS, members)),
            dma((STEPS - 1,)), dma((STEPS,)), dma((STEPS, members)),
            dma((2, n_col - 1)), dma((2, STEPS)), dma((2,)),
        ],
        compiler_params=pltpu.CompilerParams(collective_id=0, has_side_effects=True),
    )(strip_rows, strip_cols)


def finish_kernel(offset, closed, panel_rows, weights, out, low_right, high_right, low_left, high_left):
    tile, cols = weights.shape
    wide = 256

    @pl.when(pl.program_id(0) == 0)
    def _():
        def one(index, carry):
            s, part = index // (cols // wide), index % (cols // wide)
            where = pl.ds(pl.multiple_of(part * wide, wide), wide)
            low, high = encode_right(panel_rows[s, :, where].astype(jnp.float32))
            low_right[s, :, where] = low
            high_right[s, :, where] = high
            return carry

        lax.fori_loop(0, STEPS * (cols // wide), one, 0)

    for s in range(STEPS):
        low, high = encode_left(closed[s].astype(jnp.float32))
        low_left[s] = low
        high_left[s] = high

    base = offset[0] + pl.program_id(0) * tile

    def columns(index, carry):
        start = pl.multiple_of(index * wide, wide)
        where = pl.ds(start, wide)
        low = product(low_left[0], low_right[0, :, where])
        high = product(high_left[0], high_right[0, :, where])
        for s in range(1, STEPS):
            low = jnp.maximum(low, product(low_left[s], low_right[s, :, where]))
            high = jnp.maximum(high, product(high_left[s], high_right[s, :, where]))
        shape = (tile, wide)
        gap = lax.broadcasted_iota(jnp.int32, shape, 0) - lax.broadcasted_iota(jnp.int32, shape, 1)
        old = jnp.where(gap == start - base, 0, weights[:, where])
        best = jnp.minimum(decode(low, high), 64.0).astype(jnp.int32)
        out[:, where] = jnp.minimum(old, best)
        return carry

    lax.fori_loop(0, cols // wide, columns, 0)


def finish(offset, closed, panel_rows, weights):
    rows, cols = weights.shape
    tile = 256
    return pl.pallas_call(
        finish_kernel,
        out_shape=jax.ShapeDtypeStruct(weights.shape, jnp.int32),
        grid=(rows // tile,),
        in_specs=[
            pl.BlockSpec(memory_space=pltpu.SMEM),
            pl.BlockSpec((STEPS, tile, PIVOT), lambda i: (0, i, 0)),
            pl.BlockSpec((STEPS, PIVOT, cols), lambda i: (0, 0, 0)),
            pl.BlockSpec((tile, cols), lambda i: (i, 0)),
        ],
        out_specs=pl.BlockSpec((tile, cols), lambda i: (i, 0)),
        scratch_shapes=[
            pltpu.VMEM((STEPS, 2 * PIVOT, cols), jnp.bfloat16),
            pltpu.VMEM((STEPS, 4 * PIVOT, cols), jnp.bfloat16),
            pltpu.VMEM((STEPS, tile, 2 * PIVOT), jnp.bfloat16),
            pltpu.VMEM((STEPS, tile, 4 * PIVOT), jnp.bfloat16),
        ],
    )(offset, closed, panel_rows, weights)


def solution(mesh):
    n_row, n_col = mesh.shape["row"], mesh.shape["col"]
    assert n_row % STEPS == 0 and n_col % STEPS == 0

    def per_device(weights):
        rows_dev, cols_dev = weights.shape
        offset = lax.axis_index("row") * rows_dev - lax.axis_index("col") * cols_dev
        offset = jnp.full((1,), offset, jnp.int32)
        panel_rows, closed = gather_close(n_row, n_col, *strips(offset, weights))
        return finish(offset, closed, panel_rows, weights)

    return jax.shard_map(
        per_device, mesh=mesh, in_specs=(P("row", "col"),), out_specs=P("row", "col"), check_vma=False)
```

```python
import jax
import jax.numpy as jnp
from jax import lax
from jax.experimental import pallas as pl
from jax.experimental.pallas import tpu as pltpu
from jax.sharding import PartitionSpec as P

PIVOT = 128
STEPS = 4
MESH = pl.DeviceIdType.MESH

BETA = 7.03
SLACK = 0.0021
LOW_SUM = 18.19
HIGH_LEFT = ((18.09, 0, 36), (35.09, 17, 36), (8.09, 0, 26), (45.09, 37, 63))
HIGH_RIGHT = ((35.09, 17, 53), (18.09, 0, 16), (45.09, 54, 63), (8.09, 0, 26))
HIGH_SUM = 53.18
HIGH_FIRST = 36.0


def step_of(centre, base):
    return 2.0 ** (BETA * (centre - base))


def power(scaled, centre):
    return jnp.exp2(BETA * centre - scaled)


def keep(value, dist, first, last):
    dist = dist.astype(jnp.bfloat16)
    kept = dist <= last if first == 0 else (dist >= first) & (dist <= last)
    return jnp.where(kept, value.astype(jnp.bfloat16), jnp.bfloat16(0))


def encode_left(dist):
    scaled = dist * BETA
    p18 = power(scaled, 18.09)
    p08 = p18 * step_of(8.09, 18.09)
    first = keep(p18, dist, 0, 36)
    low = [first, keep(p08 * step_of(0.10, 8.09), dist, 0, 17)]
    high = [first, keep(p18 * step_of(35.09, 18.09), dist, 17, 36), keep(p08, dist, 0, 26),
            keep(power(scaled, 45.09), dist, 37, 63)]
    return jnp.concatenate(low, axis=1), jnp.concatenate(high, axis=1)


def encode_right(dist):
    scaled = dist * BETA
    p18 = power(scaled, 18.09)
    p08 = p18 * step_of(8.09, 18.09)
    low = [keep(p08 * step_of(0.10, 8.09), dist, 0, 17), keep(p18, dist, 18, 36)]
    high = [keep(power(scaled, 35.09), dist, 17, 53), keep(p18, dist, 0, 16),
            keep(power(scaled, 45.09), dist, 54, 63), keep(p08, dist, 0, 26)]
    return jnp.concatenate(low, axis=0), jnp.concatenate(high, axis=0)


def product(left, right):
    return jnp.dot(left, right, preferred_element_type=jnp.float32)


def decode(low, high):
    low = (LOW_SUM - SLACK) - jnp.log2(low) * (1.0 / BETA)
    high = (HIGH_SUM - SLACK) - jnp.log2(high) * (1.0 / BETA)
    return jnp.ceil(jnp.minimum(low, jnp.maximum(high, HIGH_FIRST)))


def min_plus(left, right):
    return decode(product(left[0], right[0]), product(left[1], right[1]))


def strips_kernel(offset, rows, cols, strip_rows, strip_cols):
    for part, strip in ((rows, strip_rows), (cols, strip_cols)):
        gap = lax.broadcasted_iota(jnp.int32, part.shape, 0) - lax.broadcasted_iota(jnp.int32, part.shape, 1)
        kept = jnp.where(gap == -offset[0], 0, part[...])
        strip[...] = kept.astype(jnp.float32).astype(jnp.bfloat16)


def strips(offset, weights):
    rows, cols = weights.shape
    corner = lambda shape: pl.BlockSpec(shape, lambda i: (0, 0))
    shapes = (PIVOT, cols), (rows, PIVOT)
    return pl.pallas_call(
        strips_kernel,
        out_shape=tuple(jax.ShapeDtypeStruct(shape, jnp.bfloat16) for shape in shapes),
        grid=(1,),
        in_specs=[pl.BlockSpec(memory_space=pltpu.SMEM)] + [corner(shape) for shape in shapes],
        out_specs=tuple(corner(shape) for shape in shapes),
    )(offset, weights, weights)


def close_block(block):
    def square(_, now):
        return jnp.minimum(now, min_plus(encode_left(now), encode_right(now)))

    return lax.fori_loop(0, 6, square, block)


def gather_close_kernel(n_row, n_col, strip_rows, strip_cols, panel_rows, closed,
                        panel_cols, pivots, dist, low_right, high_right,
                        send_piv, recv_piv, pass_piv, send_rows, recv_rows, pass_rows,
                        send_cols, recv_cols, local_sem):
    r, c = lax.axis_index("row"), lax.axis_index("col")
    row_gap, col_gap = n_row // STEPS, n_col // STEPS
    leader = lax.rem(r, row_gap) == 0
    group = r // row_gap
    rows_dev = strip_cols.shape[0]
    barrier = pltpu.get_barrier_semaphore()
    for k in range(1, n_row):
        pl.semaphore_signal(barrier, inc=1, device_id=(lax.rem(r + k, n_row), c), device_id_type=MESH)
    for k in range(1, n_col):
        pl.semaphore_signal(barrier, inc=1, device_id=(r, lax.rem(c + k, n_col)), device_id_type=MESH)
    pl.semaphore_wait(barrier, n_row + n_col - 2)

    parts = pl.ds(0, PIVOT), pl.ds(PIVOT, rows_dev - PIVOT)

    def cols_copy(s, part, k):
        return pltpu.make_async_remote_copy(
            src_ref=strip_cols.at[parts[part]], dst_ref=panel_cols.at[s, parts[part]],
            send_sem=send_cols.at[part, k - 1], recv_sem=recv_cols.at[part, s],
            device_id=(r, lax.rem(c + k, n_col)), device_id_type=MESH)

    def cols_own(s, part):
        return pltpu.make_async_copy(
            strip_cols.at[parts[part]], panel_cols.at[s, parts[part]], local_sem.at[part])

    def to_leader(src, dst, s, k, send, recv):
        return pltpu.make_async_remote_copy(
            src_ref=src, dst_ref=dst.at[s], send_sem=send.at[k - 1], recv_sem=recv.at[s],
            device_id=(lax.rem(r + k * row_gap, n_row), c), device_id_type=MESH)

    def to_member(src, dst, s, m, send, recv):
        return pltpu.make_async_remote_copy(
            src_ref=src, dst_ref=dst.at[s], send_sem=send.at[s, m - 1], recv_sem=recv.at[s],
            device_id=(r + m, c), device_id_type=MESH)

    corner = panel_cols.at[:, parts[0]]
    piv = pivots, send_piv, recv_piv
    row = panel_rows, send_rows, recv_rows

    for s in range(STEPS):
        @pl.when(c == s * col_gap)
        def _():
            @pl.when(leader)
            def _():
                for k in range(1, n_col):
                    cols_copy(s, 0, k).start()
            cols_own(s, 0).start()
            cols_own(s, 1).start()
            cols_own(s, 0).wait()
            cols_own(s, 1).wait()

    for s in range(STEPS):
        @pl.when(leader & (c != s * col_gap))
        def _():
            cols_copy(s, 0, 1).wait_recv()

    for s in range(STEPS):
        @pl.when(leader & (group == s))
        def _():
            for k in range(1, STEPS):
                to_leader(corner, pivots, s, k, send_piv, recv_piv).start()
            for m in range(1, row_gap):
                to_member(corner, pivots, s, m, pass_piv, recv_piv).start()
            for k in range(1, STEPS):
                to_leader(strip_rows, panel_rows, s, k, send_rows, recv_rows).start()
            for m in range(1, row_gap):
                to_member(strip_rows, panel_rows, s, m, pass_rows, recv_rows).start()
            own_piv = pltpu.make_async_copy(corner, pivots.at[s], local_sem.at[0])
            own_row = pltpu.make_async_copy(strip_rows, panel_rows.at[s], local_sem.at[1])
            own_piv.start()
            own_row.start()
            own_piv.wait()
            own_row.wait()

    for s in range(STEPS):
        @pl.when(leader & (c == s * col_gap))
        def _():
            for k in range(1, n_col):
                cols_copy(s, 1, k).start()

    def pass_on(dst, passing, send, recv):
        for j in range(1, STEPS):
            s = lax.rem(group + j, STEPS)

            @pl.when(leader)
            def _():
                to_leader(dst.at[0], dst, s, 1, send, recv).wait_recv()
                for m in range(1, row_gap):
                    to_member(dst.at[s], dst, s, m, passing, recv).start()

    pass_on(pivots, pass_piv, send_piv, recv_piv)

    @pl.when(jnp.logical_not(leader))
    def _():
        for s in range(STEPS):
            to_member(pivots.at[s], pivots, s, 1, pass_piv, recv_piv).wait_recv()

    for s in range(STEPS):
        @pl.when(jnp.logical_not(leader) & (c == s * col_gap))
        def _():
            for part in range(2):
                for k in range(1, n_col):
                    cols_copy(s, part, k).start()

    size = STEPS * PIVOT
    for s in range(STEPS):
        for t in range(STEPS):
            dist[s * PIVOT : (s + 1) * PIVOT, t * PIVOT : (t + 1) * PIVOT] = pivots[s, t].astype(jnp.float32)
    for s in range(STEPS):
        mine = slice(s * PIVOT, (s + 1) * PIVOT)
        block = close_block(dist[mine, mine])
        column = min_plus(encode_left(dist[:, mine]), encode_right(block))
        dist[...] = jnp.minimum(dist[...], min_plus(encode_left(column), encode_right(dist[mine, :])))
        if s == STEPS // 2 - 1:
            pass_on(panel_rows, pass_rows, send_rows, recv_rows)

    for s in range(STEPS):
        low, high = encode_right(dist[s * PIVOT : (s + 1) * PIVOT, :])
        low_right[s] = low
        high_right[s] = high

    for s in range(STEPS):
        @pl.when(c != s * col_gap)
        def _():
            cols_copy(s, 1, 1).wait_recv()

        @pl.when(jnp.logical_not(leader) & (c != s * col_gap))
        def _():
            cols_copy(s, 0, 1).wait_recv()

    tile = 256

    def update(index, carry):
        part = pl.ds(pl.multiple_of(index * tile, tile), tile)
        low = high = None
        for s in range(STEPS):
            left = encode_left(panel_cols[s, part, :].astype(jnp.float32))
            one, two = product(left[0], low_right[s]), product(left[1], high_right[s])
            low = one if s == 0 else jnp.maximum(low, one)
            high = two if s == 0 else jnp.maximum(high, two)
        best = jnp.minimum(decode(low, high), 64.0).astype(jnp.bfloat16)
        for s in range(STEPS):
            closed[s, part, :] = best[:, s * PIVOT : (s + 1) * PIVOT]
        return carry

    lax.fori_loop(0, rows_dev // tile, update, 0, unroll=True)

    @pl.when(jnp.logical_not(leader))
    def _():
        for s in range(STEPS):
            to_member(panel_rows.at[s], panel_rows, s, 1, pass_rows, recv_rows).wait_recv()

    for s in range(STEPS):
        @pl.when(c == s * col_gap)
        def _():
            for part in range(2):
                for k in range(1, n_col):
                    cols_copy(s, part, k).wait_send()

        @pl.when(leader)
        def _():
            for m in range(1, row_gap):
                to_member(pivots.at[s], pivots, s, m, pass_piv, recv_piv).wait_send()
                to_member(panel_rows.at[s], panel_rows, s, m, pass_rows, recv_rows).wait_send()

    @pl.when(leader)
    def _():
        for k in range(1, STEPS):
            to_leader(corner, pivots, 0, k, send_piv, recv_piv).wait_send()
            to_leader(strip_rows, panel_rows, 0, k, send_rows, recv_rows).wait_send()


def gather_close(n_row, n_col, strip_rows, strip_cols):
    rows_dev, cols_dev = strip_cols.shape[0], strip_rows.shape[1]
    vmem = pl.BlockSpec(memory_space=pltpu.VMEM)
    dma = pltpu.SemaphoreType.DMA
    size = STEPS * PIVOT
    members = max(n_row // STEPS - 1, 1)
    return pl.pallas_call(
        lambda *refs: gather_close_kernel(n_row, n_col, *refs),
        out_shape=(
            jax.ShapeDtypeStruct((STEPS, PIVOT, cols_dev), jnp.bfloat16),
            jax.ShapeDtypeStruct((STEPS, rows_dev, PIVOT), jnp.bfloat16),
        ),
        in_specs=[vmem] * 2,
        out_specs=(vmem,) * 2,
        scratch_shapes=[
            pltpu.VMEM((STEPS, rows_dev, PIVOT), jnp.bfloat16),
            pltpu.VMEM((STEPS, STEPS, PIVOT, PIVOT), jnp.bfloat16),
            pltpu.VMEM((size, size), jnp.float32),
            pltpu.VMEM((STEPS, 2 * PIVOT, size), jnp.bfloat16),
            pltpu.VMEM((STEPS, 4 * PIVOT, size), jnp.bfloat16),
            dma((STEPS - 1,)), dma((STEPS,)), dma((STEPS, members)),
            dma((STEPS - 1,)), dma((STEPS,)), dma((STEPS, members)),
            dma((2, n_col - 1)), dma((2, STEPS)), dma((2,)),
        ],
        compiler_params=pltpu.CompilerParams(collective_id=0, has_side_effects=True),
    )(strip_rows, strip_cols)


def finish_kernel(offset, closed, panel_rows, weights, out, low_right, high_right, low_left, high_left):
    tile, cols = weights.shape
    wide = 256

    @pl.when(pl.program_id(0) == 0)
    def _():
        def one(index, carry):
            s, part = index // (cols // wide), index % (cols // wide)
            where = pl.ds(pl.multiple_of(part * wide, wide), wide)
            low, high = encode_right(panel_rows[s, :, where].astype(jnp.float32))
            low_right[s, :, where] = low
            high_right[s, :, where] = high
            return carry

        lax.fori_loop(0, STEPS * (cols // wide), one, 0, unroll=2)

    for s in range(STEPS):
        low, high = encode_left(closed[s].astype(jnp.float32))
        low_left[s] = low
        high_left[s] = high

    base = offset[0] + pl.program_id(0) * tile

    def columns(index, carry):
        start = pl.multiple_of(index * wide, wide)
        where = pl.ds(start, wide)
        low = product(low_left[0], low_right[0, :, where])
        high = product(high_left[0], high_right[0, :, where])
        for s in range(1, STEPS):
            low = jnp.maximum(low, product(low_left[s], low_right[s, :, where]))
            high = jnp.maximum(high, product(high_left[s], high_right[s, :, where]))
        shape = (tile, wide)
        gap = lax.broadcasted_iota(jnp.int32, shape, 0) - lax.broadcasted_iota(jnp.int32, shape, 1)
        old = jnp.where(gap == start - base, 0, weights[:, where])
        best = jnp.minimum(decode(low, high), 64.0).astype(jnp.int32)
        out[:, where] = jnp.minimum(old, best)
        return carry

    lax.fori_loop(0, cols // wide, columns, 0, unroll=2)


def finish(offset, closed, panel_rows, weights):
    rows, cols = weights.shape
    tile = 256
    return pl.pallas_call(
        finish_kernel,
        out_shape=jax.ShapeDtypeStruct(weights.shape, jnp.int32),
        grid=(rows // tile,),
        in_specs=[
            pl.BlockSpec(memory_space=pltpu.SMEM),
            pl.BlockSpec((STEPS, tile, PIVOT), lambda i: (0, i, 0)),
            pl.BlockSpec((STEPS, PIVOT, cols), lambda i: (0, 0, 0)),
            pl.BlockSpec((tile, cols), lambda i: (i, 0)),
        ],
        out_specs=pl.BlockSpec((tile, cols), lambda i: (i, 0)),
        scratch_shapes=[
            pltpu.VMEM((STEPS, 2 * PIVOT, cols), jnp.bfloat16),
            pltpu.VMEM((STEPS, 4 * PIVOT, cols), jnp.bfloat16),
            pltpu.VMEM((STEPS, tile, 2 * PIVOT), jnp.bfloat16),
            pltpu.VMEM((STEPS, tile, 4 * PIVOT), jnp.bfloat16),
        ],
    )(offset, closed, panel_rows, weights)


def solution(mesh):
    n_row, n_col = mesh.shape["row"], mesh.shape["col"]
    assert n_row % STEPS == 0 and n_col % STEPS == 0

    def per_device(weights):
        rows_dev, cols_dev = weights.shape
        offset = lax.axis_index("row") * rows_dev - lax.axis_index("col") * cols_dev
        offset = jnp.full((1,), offset, jnp.int32)
        panel_rows, closed = gather_close(n_row, n_col, *strips(offset, weights))
        return finish(offset, closed, panel_rows, weights)

    return jax.shard_map(
        per_device, mesh=mesh, in_specs=(P("row", "col"),), out_specs=P("row", "col"), check_vma=False)
```
